32 devices in a mesh: clip: 2 (over y), ha: 8 (over z, x), ta: 2 (over core).
Axes of the slice: x: 2, y: 2, z: 4, core: 2. Of those that a mesh axis runs over, the one named last changes fastest.
Arguments:
- latent_tokens: bfloat16 [16, 512, 64], P('clip', ('ha', 'ta')), parts along dimension 0, may hold values from -8 to 8
- w_in: bfloat16 [3, 3, 3, 16, 384], replicated, may hold values from -0.3125 to 0.3125
- b_in: float32 [384], replicated, may hold values from -3 to 3
- gn_gain: float32 [384], replicated, may hold values from 0.1 to 1.9
- gn_shift: float32 [384], replicated, may hold values from -3 to 3
- w_mid: bfloat16 [3, 3, 3, 384, 384], replicated, may hold values from -0.109375 to 0.109375
- b_mid: float32 [384], replicated, may hold values from -3 to 3
Outputs:
- decoded: bfloat16 [16, 16, 128, 384], P(('clip', 'ta'), 'ha'), parts along dimension 0
The draws below stay inside these ranges and needn't reach their ends.
There are 2 independent parts, one for each index of `clip`. The reference program is written for one: setup_inputs(seed, part) draws one part's arguments, and reference() takes and returns one part's arrays. A program takes and returns all parts, laid end to end along the dimension named above; an argument that names none is the same for every part. Nothing has to cross between parts.
All inputs are finite; a program needn't handle non-finite values.
Results may differ from the reference program's by a relative error of at most 0.0054.
Values may be sent and summed in bfloat16 or wider, within the bound.
A program may use at most 64 MiB of HBM per device.

```python
import jax
import jax.numpy as jnp
from jax import lax

CH = 384
ZC = 16
GROUPS = 32
W = 128
FRAMES = 8
ROWS = 16
TOKENS_F = 512


def draw_latent_tokens(key, part):
    keys = jax.random.split(key, 3)
    token = jnp.arange(TOKENS_F)
    entry = jnp.arange(4 * ZC)
    row_index = 2 * (token // (W // 2))[:, None] + (entry // (2 * ZC))[None, :]
    channel = entry % ZC
    rough = jnp.exp(jax.random.uniform(keys[0], (FRAMES, ROWS), minval=-1.15, maxval=1.15))
    chan_scale = jnp.exp(jax.random.uniform(keys[1], (ZC,), minval=-0.7, maxval=0.7))
    position = row_index.astype(jnp.float32) / max(ROWS - 1, 1)
    trend = 0.6 + 1.2 * position
    base = jax.random.normal(keys[2], (FRAMES, TOKENS_F, 4 * ZC))
    scale = 0.4 * rough[:, row_index] * trend[None] * chan_scale[channel][None, None, :]
    value = base * scale
    return jnp.clip(value, -8.0, 8.0).astype(jnp.bfloat16)


def gaussian(stream_key, extent, width, most, dtype=jnp.bfloat16):
    values = jax.random.normal(stream_key, extent, jnp.float32) * width
    return jnp.minimum(jnp.maximum(values, -most), most).astype(dtype)


def setup_inputs(seed: int = 0, part: int = 0) -> dict:
    splits = jax.random.split(jax.random.key(seed), 8)
    own_keys = jax.random.split(jax.random.fold_in(splits[7], part), 8)
    return {
        "latent_tokens": draw_latent_tokens(jax.random.fold_in(jax.random.fold_in(splits[7], part), 71), part),
        "w_in": gaussian(splits[1], (3, 3, 3, ZC, CH), (27 * ZC) ** -0.5, 0.3125),
        "b_in": gaussian(splits[2], (CH,), 0.5, 3.0, jnp.float32),
        "gn_gain": jnp.clip(1.0 + 0.18 * jax.random.normal(splits[3], (CH,), jnp.float32), 0.1, 1.9),
        "gn_shift": gaussian(splits[4], (CH,), 0.5, 3.0, jnp.float32),
        "w_mid": gaussian(splits[5], (3, 3, 3, CH, CH), (9 * CH) ** -0.5, 0.109375),
        "b_mid": gaussian(splits[6], (CH,), 0.5, 3.0, jnp.float32),
    }


def causal_conv(field, kernel):
    result = lax.conv_general_dilated(field[None].astype(jnp.float32), kernel.astype(jnp.float32), (1, 1, 1), [(2, 0), (1, 1), (1, 1)], dimension_numbers=('NDHWC', 'DHWIO', 'NDHWC'), precision=lax.Precision.HIGHEST)
    return result[0]

def reference(latent_tokens, w_in, b_in, gn_gain, gn_shift, w_mid, b_mid):
    latent = latent_tokens.reshape(FRAMES, ROWS // 2, W // 2, 2, 2, ZC)
    latent = latent.transpose(0, 1, 3, 2, 4, 5).reshape(FRAMES, ROWS, W, ZC)
    hidden = (causal_conv(latent, w_in) + b_in).astype(jnp.bfloat16)
    values = lax.optimization_barrier(hidden).astype(jnp.float32)
    grouped = values.reshape(FRAMES, ROWS, W, GROUPS, CH // GROUPS)
    mean = lax.optimization_barrier(jnp.mean(grouped, axis=(0, 1, 2, 4), keepdims=True))
    var = lax.optimization_barrier(jnp.mean((grouped - mean) * (grouped - mean), axis=(0, 1, 2, 4), keepdims=True))
    normed = ((grouped - mean) * lax.rsqrt(var + 1e-06)).reshape(FRAMES, ROWS, W, CH)
    active = jax.nn.silu(normed * gn_gain + gn_shift).astype(jnp.bfloat16)
    active = lax.optimization_barrier(active)
    branch = causal_conv(active, w_mid)
    return (values + branch + b_mid).astype(jnp.bfloat16)
```

```python
import functools

import jax
import jax.numpy as jnp
from jax import lax
from jax.experimental import pallas as pl
from jax.experimental.pallas import tpu as pltpu
from jax.sharding import PartitionSpec as P

GROUPS = 32
EPS = 1e-06
F32 = jnp.float32
BF16 = jnp.bfloat16
MESH = pl.DeviceIdType.MESH
LANES = 128


def split_dot(rows, ones):
    first = rows.astype(BF16).astype(F32)
    rest = rows - first
    second = rest.astype(BF16).astype(F32)
    third = rest - second
    stacked = jnp.concatenate([first, second, third, jnp.zeros_like(first)] * 2, axis=0)
    keep = lax.broadcasted_iota(jnp.int32, stacked.shape, 0) < 3
    stacked = jnp.where(keep, stacked, 0.0).astype(BF16)
    return jnp.sum(jnp.dot(stacked, ones, preferred_element_type=F32), axis=0, keepdims=True)


def group_of(index, members):
    return jnp.floor((index.astype(F32) + 0.5) * (1.0 / members))


def kernel(
    n_ha, n_ta, tok, w_in, b_in, gain, shift, w_mid, b_mid, out,
    pk, rx, wexp, patch, hid, act, acc, stage, wv, stat, gath, sums, spread,
    w_sem, tx_a, tx_b, rx_a, rx_b, st_tx, st_rx,
):
    h = lax.axis_index("ha")
    t = lax.axis_index("ta")
    n = n_ha * n_ta
    me = h * n_ta + t
    frames, half, width = tok.shape
    fr = frames // n_ta
    ch = b_in.shape[-1]
    members = ch // GROUPS
    cj = half * n_ta
    zc = width // 4
    ext = fr + 2

    for k in range(9):
        pltpu.make_async_copy(w_mid.at[k], wv.at[k], w_sem.at[k]).start()

    packed = jnp.concatenate([tok[:, : half // 2, :], tok[:, half // 2 :, :]], axis=-1)
    pk[...] = packed
    rx[...] = jnp.zeros_like(rx)
    rx[1, t, pl.ds(fr * (1 - t), fr)] = packed[:fr]

    @pl.when(t == 1)
    def _():
        rx[1, 1, fr:] = packed[fr:]

    barrier = pltpu.get_barrier_semaphore()

    def greet(k, c):
        peer = lax.rem(me + k, n)
        pl.semaphore_signal(
            barrier, inc=1, device_id={"ha": peer // n_ta, "ta": peer % n_ta}, device_id_type=MESH
        )
        return c

    lax.fori_loop(1, n, greet, 0)

    zero = jnp.zeros((zc, ch), BF16)
    for p in range(3):
        for block in range(4):
            for a1 in range(2):
                for b1 in range(2):
                    dy = (-1 if a1 else 2) if block >= 2 else a1
                    dx = (-1 if b1 else 2) if block % 2 else b1
                    row = p * 16 * zc + block * 4 * zc + (2 * a1 + b1) * zc
                    for a in range(2):
                        for b in range(2):
                            q, r = dy - a + 1, dx - b + 1
                            inside = 0 <= q <= 2 and 0 <= r <= 2
                            piece = w_in[3 * p + q, r * zc : (r + 1) * zc, :] if inside else zero
                            col = (2 * a + b) * ch
                            wexp[row : row + zc, col : col + ch] = piece
    chan = lax.broadcasted_iota(jnp.int32, (ch, ch + LANES), 0)
    lane = lax.broadcasted_iota(jnp.int32, (ch, ch + LANES), 1)
    target = jnp.where(lane < ch, group_of(lane, members), (lane - ch).astype(F32))
    sums[...] = jnp.where(group_of(chan, members) == target, 1.0, 0.0).astype(BF16)
    chan = lax.broadcasted_iota(jnp.int32, (LANES, ch), 1)
    lane = lax.broadcasted_iota(jnp.int32, (LANES, ch), 0)
    spread[...] = jnp.where(group_of(chan, members) == lane.astype(F32), 1.0, 0.0).astype(BF16)

    pl.semaphore_wait(barrier, n - 1)

    partners = [(0, 1), (1, 0), (-1, 0), (1, 1), (-1, 1)]

    def copies(s):
        dh, dt = partners[s]
        other = (t + dt) % n_ta
        to = {"ha": h + dh, "ta": other}
        first = pltpu.make_async_remote_copy(
            src_ref=pk.at[pl.ds(0, fr)],
            dst_ref=rx.at[1 - dh, t, pl.ds(fr * (1 - other), fr)],
            send_sem=tx_a.at[s], recv_sem=rx_a.at[s], device_id=to, device_id_type=MESH,
        )
        second = pltpu.make_async_remote_copy(
            src_ref=pk.at[pl.ds(fr, fr)],
            dst_ref=rx.at[1 - dh, t, pl.ds(fr, fr)],
            send_sem=tx_b.at[s], recv_sem=rx_b.at[s], device_id=to, device_id_type=MESH,
        )
        return first, second, other

    def exists(s, sign):
        dh = partners[s][0] * sign
        return jnp.logical_and(h + dh >= 0, h + dh < n_ha)

    for s in range(5):

        @pl.when(exists(s, 1))
        def _(s=s):
            first, second, other = copies(s)
            first.start()

            @pl.when(other == 1)
            def _():
                second.start()

    for s in range(5):

        @pl.when(exists(s, -1))
        def _(s=s):
            first, second, _ = copies(s)
            first.wait_recv()

            @pl.when(t == 1)
            def _():
                second.wait_recv()

    rows = frames * cj
    j = lax.broadcasted_iota(jnp.int32, (rows, width), 0) & (cj - 1)
    lane = lax.broadcasted_iota(jnp.int32, (rows, width), 1)
    upper_b = (lane & zc) != 0
    wide = []
    for i in range(3):
        parts = []
        for side in range(n_ta):
            held = rx[i, side].astype(F32)
            parts += [held[:, :, :width], held[:, :, width:]]
        field = jnp.concatenate(parts, axis=1).reshape(rows, width)
        left = jnp.where(j == 0, 0.0, pltpu.roll(field, 1, 0))
        right = jnp.where(j == cj - 1, 0.0, pltpu.roll(field, rows - 1, 0))
        wide.append(jnp.concatenate([field, jnp.where(upper_b, left, right)], axis=-1))
    lane = lax.broadcasted_iota(jnp.int32, (rows, 2 * width), 1)
    upper_a = (lane & (2 * zc)) != 0
    nothing = jnp.zeros_like(wide[0])
    for i in range(3):
        above = wide[i - 1] if i > 0 else nothing
        below = wide[i + 1] if i < 2 else nothing
        crossed = jnp.where(upper_a, above, below)
        patch[i, :, : 2 * width] = wide[i].astype(BF16)
        patch[i, :, 2 * width :] = crossed.astype(BF16)

    def conv(i, lo, count, col0, ncol):
        lhs = jnp.concatenate(
            [patch[i, (lo + p) * cj : (lo + p + count) * cj, :] for p in range(3)], axis=-1
        )
        got = jnp.dot(lhs, wexp[:, col0 : col0 + ncol], preferred_element_type=F32)
        results = []
        for piece in range(ncol // ch):
            value = (got[:, piece * ch : (piece + 1) * ch] + b_in[...]).astype(BF16)
            results.append(value)
        return results

    own = conv(1, 2, fr, 0, 4 * ch)
    total = jnp.zeros((1, ch), F32)
    for ab in range(4):
        hid[2:, 1 + ab // 2, ab % 2] = own[ab].reshape(fr, cj, ch)
        total = total + jnp.sum(own[ab].astype(F32), axis=0, keepdims=True)
    cells = 4 * fr * cj
    chan_mean = total * (1.0 / cells)
    squares = jnp.zeros((1, ch), F32)
    for ab in range(4):
        value = hid[2:, 1 + ab // 2, ab % 2].reshape(fr * cj, ch).astype(F32) - chan_mean
        squares = squares + jnp.sum(value * value, axis=0, keepdims=True)
    grouped = split_dot(chan_mean, sums[...]) * (1.0 / members)
    apart = chan_mean - grouped[:, :ch]
    local_m2 = split_dot(squares + cells * apart * apart, sums[:, ch:])
    stat[...] = jnp.concatenate([grouped[:, ch:], local_m2], axis=0)
    gath[me] = stat[...]

    def share(k, c):
        peer = lax.rem(me + k, n)
        pltpu.make_async_remote_copy(
            src_ref=stat, dst_ref=gath.at[me], send_sem=st_tx, recv_sem=st_rx,
            device_id={"ha": peer // n_ta, "ta": peer % n_ta}, device_id_type=MESH,
        ).start()
        return c

    lax.fori_loop(1, n, share, 0)

    early = conv(1, 0, 2, 0, 4 * ch)
    for ab in range(4):
        hid[:2, 1 + ab // 2, ab % 2] = early[ab].reshape(2, cj, ch)
    over = conv(0, 0, ext, 2 * ch, 2 * ch)
    under = conv(2, 0, ext, 0, 2 * ch)
    for b in range(2):
        hid[:, 0, b] = over[b].reshape(ext, cj, ch)
        hid[:, 3, b] = under[b].reshape(ext, cj, ch)

    others = gath.at[pl.ds(0, n - 1)]
    pltpu.make_async_copy(others, others, st_rx).wait()
    pltpu.make_async_copy(others, others, st_tx).wait()
    for s in range(5):

        @pl.when(exists(s, 1))
        def _(s=s):
            first, second, other = copies(s)
            first.wait_send()

            @pl.when(other == 1)
            def _():
                second.wait_send()

    every = gath[...]
    means = every[:, 0:1, :]
    mean = jnp.sum(means, axis=0) * (1.0 / n)
    gap = means - mean[None]
    count = float(cells * members)
    m2 = jnp.sum(every[:, 1:2, :], axis=0) + count * jnp.sum(gap * gap, axis=0)
    mean_c = split_dot(mean, spread[...])
    var_c = split_dot(m2 * (1.0 / (count * n)), spread[...])
    scale_c = lax.rsqrt(var_c + EPS) * gain[...]

    j = lax.broadcasted_iota(jnp.int32, (cj, ch), 0)

    def activate(k, c):
        lf, y = k // 4, k % 4
        good = jnp.logical_and(
            t * fr + lf >= 2, jnp.logical_and(h * 2 + y >= 1, h * 2 + y < 2 * n_ha + 1)
        )
        live = jnp.where(good, 0.5, 0.0)
        pair = []
        for b in range(2):
            v = (hid[lf, y, b].astype(F32) - mean_c) * scale_c + shift[...]
            pair.append((v * live) * (1.0 + jnp.tanh(0.5 * v)))
        even, odd = pair
        odd_left = jnp.where(j == 0, 0.0, pltpu.roll(odd, 1, 0)).astype(BF16)
        even_right = jnp.where(j == cj - 1, 0.0, pltpu.roll(even, cj - 1, 0)).astype(BF16)
        even, odd = even.astype(BF16), odd.astype(BF16)
        for b, pieces in enumerate(((odd_left, even, odd), (even, odd, even_right))):
            for r in range(3):
                act[lf, y, b * cj : (b + 1) * cj, r * ch : (r + 1) * ch] = pieces[r]
        return c

    lax.fori_loop(0, ext * 4, activate, 0)

    acc[...] = jnp.zeros_like(acc)

    def tap(k, c):
        pltpu.make_async_copy(w_mid.at[k], wv.at[k], w_sem.at[k]).wait()
        lhs = act[pl.ds(k // 3, fr), pl.ds(k % 3, 2)].reshape(fr * 4 * cj, 3 * ch)
        acc[...] += jnp.dot(lhs, wv[k], preferred_element_type=F32)
        return c

    lax.fori_loop(0, 9, tap, 0)

    for f in range(fr):
        for y in range(2):
            base = (f * 2 + y) * 2 * cj
            for b in range(2):
                value = acc[base + b * cj : base + (b + 1) * cj, :] + b_mid[...]
                value = value + hid[f + 2, y + 1, b].astype(F32)
                for piece in range(ch // LANES):
                    cols = slice(piece * LANES, (piece + 1) * LANES)
                    stage[f * 2 + y, piece, pl.ds(b, cj, 2), :] = value[:, cols]
            for piece in range(ch // LANES):
                cols = slice(piece * LANES, (piece + 1) * LANES)
                out[f, y, :, cols] = stage[f * 2 + y, piece].astype(BF16)


def body(n_ha, n_ta, latent_tokens, w_in, b_in, gn_gain, gn_shift, w_mid, b_mid):
    frames, half, width = latent_tokens.shape
    ch = b_in.shape[0]
    zc = width // 4
    fr, cj, n = frames // n_ta, half * n_ta, n_ha * n_ta
    vm = pl.BlockSpec(memory_space=pltpu.VMEM)
    row = lambda v: v.reshape(1, ch)
    return pl.pallas_call(
        functools.partial(kernel, n_ha, n_ta),
        out_shape=jax.ShapeDtypeStruct((fr, 2, 2 * cj, ch), BF16),
        in_specs=[vm, vm, vm, vm, vm, pl.BlockSpec(memory_space=pl.ANY), vm],
        out_specs=vm,
        scratch_shapes=[
            pltpu.VMEM((frames, half // 2, 2 * width), BF16),
            pltpu.VMEM((3, n_ta, frames, half // 2, 2 * width), BF16),
            pltpu.VMEM((48 * zc, 4 * ch), BF16),
            pltpu.VMEM((3, frames * cj, 4 * width), BF16),
            pltpu.VMEM((fr + 2, 4, 2, cj, ch), BF16),
            pltpu.VMEM((fr + 2, 4, 2 * cj, 3 * ch), BF16),
            pltpu.VMEM((fr * 4 * cj, ch), F32),
            pltpu.VMEM((fr * 2, ch // LANES, 2 * cj, LANES), F32),
            pltpu.VMEM((9, 3 * ch, ch), BF16),
            pltpu.VMEM((2, LANES), F32),
            pltpu.VMEM((n, 2, LANES), F32),
            pltpu.VMEM((ch, ch + LANES), BF16),
            pltpu.VMEM((LANES, ch), BF16),
            pltpu.SemaphoreType.DMA((9,)),
            pltpu.SemaphoreType.DMA((5,)),
            pltpu.SemaphoreType.DMA((5,)),
            pltpu.SemaphoreType.DMA((5,)),
            pltpu.SemaphoreType.DMA((5,)),
            pltpu.SemaphoreType.DMA,
            pltpu.SemaphoreType.DMA,
        ],
        compiler_params=pltpu.CompilerParams(
            collective_id=0, has_side_effects=True, vmem_limit_bytes=60 * 1024 * 1024
        ),
    )(
        latent_tokens, w_in.reshape(9, 3 * zc, ch), row(b_in), row(gn_gain), row(gn_shift),
        w_mid.reshape(9, 3 * ch, ch), row(b_mid),
    )


def solution(mesh):
    placed = (P("clip", ("ha", "ta"), None), P(), P(), P(), P(), P(), P())
    return jax.shard_map(
        functools.partial(body, mesh.shape["ha"], mesh.shape["ta"]),
        mesh=mesh,
        in_specs=placed,
        out_specs=P(("clip", "ta"), "ha", None, None),
        check_vma=False,
    )
```

```python
import functools

import jax
import jax.numpy as jnp
from jax import lax
from jax.experimental import pallas as pl
from jax.experimental.pallas import tpu as pltpu
from jax.sharding import PartitionSpec as P

GROUPS = 32
EPS = 1e-06
F32 = jnp.float32
BF16 = jnp.bfloat16
MESH = pl.DeviceIdType.MESH
LANES = 128


def split_dot(rows, ones):
    first = rows.astype(BF16).astype(F32)
    rest = rows - first
    second = rest.astype(BF16).astype(F32)
    third = rest - second
    stacked = jnp.concatenate([first, second, third, jnp.zeros_like(first)] * 2, axis=0)
    keep = lax.broadcasted_iota(jnp.int32, stacked.shape, 0) < 3
    stacked = jnp.where(keep, stacked, 0.0).astype(BF16)
    return jnp.sum(jnp.dot(stacked, ones, preferred_element_type=F32), axis=0, keepdims=True)


def group_of(index, members):
    return jnp.floor((index.astype(F32) + 0.5) * (1.0 / members))


def kernel(
    n_ha, n_ta, tok, w_in, b_in, gain, shift, w_mid, b_mid, out,
    pk, rx, wexp, patch, hid, act, stage, wv, stat, gath, sums, spread,
    w_sem, tx_a, tx_b, rx_a, rx_b, st_tx, st_rx,
):
    h = lax.axis_index("ha")
    t = lax.axis_index("ta")
    n = n_ha * n_ta
    me = h * n_ta + t
    frames, half, width = tok.shape
    fr = frames // n_ta
    ch = b_in.shape[-1]
    members = ch // GROUPS
    cj = half * n_ta
    zc = width // 4
    ext = fr + 2
    b_in_c, gain_c, shift_c, b_mid_c = [v[...].reshape(1, ch) for v in (b_in, gain, shift, b_mid)]

    for k in range(9):
        pltpu.make_async_copy(w_mid.at[k], wv.at[k], w_sem.at[k]).start()

    packed = jnp.concatenate([tok[:, : half // 2, :], tok[:, half // 2 :, :]], axis=-1)
    pk[...] = packed
    rx[...] = jnp.zeros_like(rx)
    rx[1, t, pl.ds(fr * (1 - t), fr)] = packed[:fr]

    @pl.when(t == 1)
    def _():
        rx[1, 1, fr:] = packed[fr:]

    barrier = pltpu.get_barrier_semaphore()

    def greet(k, c):
        peer = lax.rem(me + k, n)
        pl.semaphore_signal(
            barrier, inc=1, device_id={"ha": peer // n_ta, "ta": peer % n_ta}, device_id_type=MESH
        )
        return c

    lax.fori_loop(1, n, greet, 0)

    zero = jnp.zeros((zc, ch), BF16)
    for p in range(3):
        for block in range(4):
            for a1 in range(2):
                for b1 in range(2):
                    dy = (-1 if a1 else 2) if block >= 2 else a1
                    dx = (-1 if b1 else 2) if block % 2 else b1
                    row = p * 16 * zc + block * 4 * zc + (2 * a1 + b1) * zc
                    for a in range(2):
                        for b in range(2):
                            q, r = dy - a + 1, dx - b + 1
                            inside = 0 <= q <= 2 and 0 <= r <= 2
                            piece = w_in[3 * p + q, r * zc : (r + 1) * zc, :] if inside else zero
                            col = (2 * a + b) * ch
                            wexp[row : row + zc, col : col + ch] = piece
    chan = lax.broadcasted_iota(jnp.int32, (ch, ch + LANES), 0)
    lane = lax.broadcasted_iota(jnp.int32, (ch, ch + LANES), 1)
    target = jnp.where(lane < ch, group_of(lane, members), (lane - ch).astype(F32))
    sums[...] = jnp.where(group_of(chan, members) == target, 1.0, 0.0).astype(BF16)
    chan = lax.broadcasted_iota(jnp.int32, (LANES, ch), 1)
    lane = lax.broadcasted_iota(jnp.int32, (LANES, ch), 0)
    spread[...] = jnp.where(group_of(chan, members) == lane.astype(F32), 1.0, 0.0).astype(BF16)

    pl.semaphore_wait(barrier, n - 1)

    partners = [(0, 1), (1, 0), (-1, 0), (1, 1), (-1, 1)]

    def copies(s):
        dh, dt = partners[s]
        other = (t + dt) % n_ta
        to = {"ha": h + dh, "ta": other}
        first = pltpu.make_async_remote_copy(
            src_ref=pk.at[pl.ds(0, fr)],
            dst_ref=rx.at[1 - dh, t, pl.ds(fr * (1 - other), fr)],
            send_sem=tx_a.at[s], recv_sem=rx_a.at[s], device_id=to, device_id_type=MESH,
        )
        second = pltpu.make_async_remote_copy(
            src_ref=pk.at[pl.ds(fr, fr)],
            dst_ref=rx.at[1 - dh, t, pl.ds(fr, fr)],
            send_sem=tx_b.at[s], recv_sem=rx_b.at[s], device_id=to, device_id_type=MESH,
        )
        return first, second, other

    def exists(s, sign):
        dh = partners[s][0] * sign
        return jnp.logical_and(h + dh >= 0, h + dh < n_ha)

    for s in range(5):

        @pl.when(exists(s, 1))
        def _(s=s):
            first, second, other = copies(s)
            first.start()

            @pl.when(other == 1)
            def _():
                second.start()

    for s in range(5):

        @pl.when(exists(s, -1))
        def _(s=s):
            first, second, _ = copies(s)
            first.wait_recv()

            @pl.when(t == 1)
            def _():
                second.wait_recv()

    rows = frames * cj
    j = lax.broadcasted_iota(jnp.int32, (rows, width), 0) & (cj - 1)
    lane = lax.broadcasted_iota(jnp.int32, (rows, width), 1)
    upper_b = (lane & zc) != 0
    wide = []
    for i in range(3):
        parts = []
        for side in range(n_ta):
            held = rx[i, side].astype(F32)
            parts += [held[:, :, :width], held[:, :, width:]]
        field = jnp.concatenate(parts, axis=1).reshape(rows, width)
        left = jnp.where(j == 0, 0.0, pltpu.roll(field, 1, 0))
        right = jnp.where(j == cj - 1, 0.0, pltpu.roll(field, rows - 1, 0))
        wide.append(jnp.concatenate([field, jnp.where(upper_b, left, right)], axis=-1))
    lane = lax.broadcasted_iota(jnp.int32, (rows, 2 * width), 1)
    upper_a = (lane & (2 * zc)) != 0
    nothing = jnp.zeros_like(wide[0])
    for i in range(3):
        above = wide[i - 1] if i > 0 else nothing
        below = wide[i + 1] if i < 2 else nothing
        crossed = jnp.where(upper_a, above, below)
        patch[i, :, : 2 * width] = wide[i].astype(BF16)
        patch[i, :, 2 * width :] = crossed.astype(BF16)

    def conv(i, lo, count, col0, ncol):
        lhs = jnp.concatenate(
            [patch[i, (lo + p) * cj : (lo + p + count) * cj, :] for p in range(3)], axis=-1
        )
        got = jnp.dot(lhs, wexp[:, col0 : col0 + ncol], preferred_element_type=F32)
        results = []
        for piece in range(ncol // ch):
            value = (got[:, piece * ch : (piece + 1) * ch] + b_in_c).astype(BF16)
            results.append(value)
        return results

    own = conv(1, 2, fr, 0, 4 * ch)
    total = jnp.zeros((1, ch), F32)
    for ab in range(4):
        hid[2:, 1 + ab // 2, ab % 2] = own[ab].reshape(fr, cj, ch)
        total = total + jnp.sum(own[ab].astype(F32), axis=0, keepdims=True)
    cells = 4 * fr * cj
    chan_mean = total * (1.0 / cells)
    squares = jnp.zeros((1, ch), F32)
    for ab in range(4):
        value = hid[2:, 1 + ab // 2, ab % 2].reshape(fr * cj, ch).astype(F32) - chan_mean
        squares = squares + jnp.sum(value * value, axis=0, keepdims=True)
    grouped = split_dot(chan_mean, sums[...]) * (1.0 / members)
    apart = chan_mean - grouped[:, :ch]
    local_m2 = split_dot(squares + cells * apart * apart, sums[:, ch:])
    stat[...] = jnp.concatenate([grouped[:, ch:], local_m2], axis=0)
    gath[me] = stat[...]

    def share(k, c):
        peer = lax.rem(me + k, n)
        pltpu.make_async_remote_copy(
            src_ref=stat, dst_ref=gath.at[me], send_sem=st_tx, recv_sem=st_rx,
            device_id={"ha": peer // n_ta, "ta": peer % n_ta}, device_id_type=MESH,
        ).start()
        return c

    lax.fori_loop(1, n, share, 0)

    early = conv(1, 0, 2, 0, 4 * ch)
    for ab in range(4):
        hid[:2, 1 + ab // 2, ab % 2] = early[ab].reshape(2, cj, ch)
    over = conv(0, 0, ext, 2 * ch, 2 * ch)
    under = conv(2, 0, ext, 0, 2 * ch)
    for b in range(2):
        hid[:, 0, b] = over[b].reshape(ext, cj, ch)
        hid[:, 3, b] = under[b].reshape(ext, cj, ch)

    others = gath.at[pl.ds(0, n - 1)]
    pltpu.make_async_copy(others, others, st_rx).wait()
    pltpu.make_async_copy(others, others, st_tx).wait()
    for s in range(5):

        @pl.when(exists(s, 1))
        def _(s=s):
            first, second, other = copies(s)
            first.wait_send()

            @pl.when(other == 1)
            def _():
                second.wait_send()

    every = gath[...]
    means = every[:, 0:1, :]
    mean = jnp.sum(means, axis=0) * (1.0 / n)
    gap = means - mean[None]
    count = float(cells * members)
    m2 = jnp.sum(every[:, 1:2, :], axis=0) + count * jnp.sum(gap * gap, axis=0)
    mean_c = split_dot(mean, spread[...])
    var_c = split_dot(m2 * (1.0 / (count * n)), spread[...])
    scale_c = lax.rsqrt(var_c + EPS) * gain_c

    edge = lax.broadcasted_iota(jnp.int32, (cj, ch), 0)

    def activate(lf):
        for y in range(4):
            good = jnp.logical_and(
                t * fr + lf >= 2, jnp.logical_and(h * 2 + y >= 1, h * 2 + y < 2 * n_ha + 1)
            )
            live = jnp.where(good, 0.5, 0.0)
            for b in range(2):
                v = (hid[lf, y, b].astype(F32) - mean_c) * scale_c + shift_c
                v = ((v * live) * (1.0 + jnp.tanh(0.5 * v))).astype(BF16)
                for q in range(3):
                    if 0 <= y - q < 2:
                        act[lf, y - q, b * cj : (b + 1) * cj, q * ch : (q + 1) * ch] = v

    lax.fori_loop(0, ext, lambda lf, c: (activate(lf), c)[1], 0)
    for k in range(9):
        pltpu.make_async_copy(w_mid.at[k], wv.at[k], w_sem.at[k]).wait()

    def frame(f, c):
        lhs = jnp.concatenate([act[f + p].reshape(4 * cj, 3 * ch) for p in range(3)], axis=-1)
        rhs = jnp.concatenate(
            [
                jnp.concatenate([wv[k, r * ch : (r + 1) * ch, :] for r in range(3)], axis=-1)
                for k in range(9)
            ],
            axis=0,
        )
        got = jnp.dot(lhs, rhs, preferred_element_type=F32)
        for y in range(2):
            e0, e1, e2 = [got[2 * y * cj : (2 * y + 1) * cj, r * ch : (r + 1) * ch] for r in range(3)]
            o0, o1, o2 = [
                got[(2 * y + 1) * cj : (2 * y + 2) * cj, r * ch : (r + 1) * ch] for r in range(3)
            ]
            from_left = jnp.where(edge == 0, 0.0, pltpu.roll(o0, 1, 0))
            from_right = jnp.where(edge == cj - 1, 0.0, pltpu.roll(e2, cj - 1, 0))
            for b, value in enumerate((from_left + e1 + o2, e0 + o1 + from_right)):
                value = value + (hid[f + 2, y + 1, b].astype(F32) + b_mid_c)
                for piece in range(ch // LANES):
                    cols = slice(piece * LANES, (piece + 1) * LANES)
                    stage[y, piece, pl.ds(b, cj, 2), :] = value[:, cols]
            for piece in range(ch // LANES):
                cols = slice(piece * LANES, (piece + 1) * LANES)
                out[f, y, :, cols] = stage[y, piece].astype(BF16)
        return c

    lax.fori_loop(0, fr, frame, 0)


def body(n_ha, n_ta, latent_tokens, w_in, b_in, gn_gain, gn_shift, w_mid, b_mid):
    frames, half, width = latent_tokens.shape
    ch = b_in.shape[0]
    zc = width // 4
    fr, cj, n = frames // n_ta, half * n_ta, n_ha * n_ta
    vm = pl.BlockSpec(memory_space=pltpu.VMEM)
    return pl.pallas_call(
        functools.partial(kernel, n_ha, n_ta),
        out_shape=pltpu.VMEM((fr, 2, 2 * cj, ch), BF16),
        in_specs=[vm, vm, vm, vm, vm, pl.BlockSpec(memory_space=pl.ANY), vm],
        out_specs=vm,
        scratch_shapes=[
            pltpu.VMEM((frames, half // 2, 2 * width), BF16),
            pltpu.VMEM((3, n_ta, frames, half // 2, 2 * width), BF16),
            pltpu.VMEM((48 * zc, 4 * ch), BF16),
            pltpu.VMEM((3, frames * cj, 4 * width), BF16),
            pltpu.VMEM((fr + 2, 4, 2, cj, ch), BF16),
            pltpu.VMEM((fr + 2, 2, 2 * cj, 3 * ch), BF16),
            pltpu.VMEM((2, ch // LANES, 2 * cj, LANES), F32),
            pltpu.VMEM((9, 3 * ch, ch), BF16),
            pltpu.VMEM((2, LANES), F32),
            pltpu.VMEM((n, 2, LANES), F32),
            pltpu.VMEM((ch, ch + LANES), BF16),
            pltpu.VMEM((LANES, ch), BF16),
            pltpu.SemaphoreType.DMA((9,)),
            pltpu.SemaphoreType.DMA((5,)),
            pltpu.SemaphoreType.DMA((5,)),
            pltpu.SemaphoreType.DMA((5,)),
            pltpu.SemaphoreType.DMA((5,)),
            pltpu.SemaphoreType.DMA,
            pltpu.SemaphoreType.DMA,
        ],
        compiler_params=pltpu.CompilerParams(
            collective_id=0, has_side_effects=True, vmem_limit_bytes=60 * 1024 * 1024
        ),
    )(
        latent_tokens, w_in.reshape(9, 3 * zc, ch), b_in, gn_gain, gn_shift,
        w_mid.reshape(9, 3 * ch, ch), b_mid,
    )


def solution(mesh):
    placed = (P("clip", ("ha", "ta"), None), P(), P(), P(), P(), P(), P())
    return jax.shard_map(
        functools.partial(body, mesh.shape["ha"], mesh.shape["ta"]),
        mesh=mesh,
        in_specs=placed,
        out_specs=P(("clip", "ta"), "ha", None, None),
        check_vma=False,
    )
```

```python
import functools

import jax
import jax.numpy as jnp
from jax import lax
from jax.experimental import pallas as pl
from jax.experimental.pallas import tpu as pltpu
from jax.sharding import PartitionSpec as P

GROUPS = 32
EPS = 1e-06
F32 = jnp.float32
BF16 = jnp.bfloat16
MESH = pl.DeviceIdType.MESH
LANES = 128


def split_dot(rows, ones):
    first = rows.astype(BF16).astype(F32)
    rest = rows - first
    second = rest.astype(BF16).astype(F32)
    third = rest - second
    stacked = jnp.concatenate([first, second, third, jnp.zeros_like(first)] * 2, axis=0)
    keep = lax.broadcasted_iota(jnp.int32, stacked.shape, 0) < 3
    stacked = jnp.where(keep, stacked, 0.0).astype(BF16)
    return jnp.sum(jnp.dot(stacked, ones, preferred_element_type=F32), axis=0, keepdims=True)


def group_of(index, members):
    return jnp.floor((index.astype(F32) + 0.5) * (1.0 / members))


def kernel(
    n_ha, n_ta, tok_hbm, w_in_hbm, b_in, gain, shift, w_mid, b_mid, out,
    tok, w_in, pk, rx, wexp, patch, hid, act, stage, wv, stat, gath, sums, spread,
    in_sem, w_sem, tx_a, tx_b, rx_a, rx_b, st_tx, st_rx,
):
    h = lax.axis_index("ha")
    t = lax.axis_index("ta")
    n = n_ha * n_ta
    me = h * n_ta + t
    frames, half, width = tok_hbm.shape
    fr = frames // n_ta
    ch = b_in.shape[-1]
    members = ch // GROUPS
    cj = half * n_ta
    zc = width // 4
    ext = fr + 2
    b_in_c, gain_c, shift_c, b_mid_c = [v[...].reshape(1, ch) for v in (b_in, gain, shift, b_mid)]

    get_tok = pltpu.make_async_copy(tok_hbm, tok, in_sem.at[0])
    get_w_in = pltpu.make_async_copy(w_in_hbm, w_in, in_sem.at[1])
    get_tok.start()
    rx[...] = jnp.zeros_like(rx)
    barrier = pltpu.get_barrier_semaphore()
    together = n - 1 if n <= 16 else 1

    def greet(k, c):
        peer = lax.rem(me + k, n)
        pl.semaphore_signal(
            barrier, inc=1, device_id={"ha": peer // n_ta, "ta": peer % n_ta}, device_id_type=MESH
        )
        return c

    lax.fori_loop(1, n, greet, 0, unroll=together)
    get_w_in.start()
    for k in range(9):
        pltpu.make_async_copy(w_mid.at[k], wv.at[k], w_sem.at[k]).start()

    chan = lax.broadcasted_iota(jnp.int32, (ch, ch + LANES), 0)
    lane = lax.broadcasted_iota(jnp.int32, (ch, ch + LANES), 1)
    target = jnp.where(lane < ch, group_of(lane, members), (lane - ch).astype(F32))
    sums[...] = jnp.where(group_of(chan, members) == target, 1.0, 0.0).astype(BF16)
    chan = lax.broadcasted_iota(jnp.int32, (LANES, ch), 1)
    lane = lax.broadcasted_iota(jnp.int32, (LANES, ch), 0)
    spread[...] = jnp.where(group_of(chan, members) == lane.astype(F32), 1.0, 0.0).astype(BF16)

    get_tok.wait()
    packed = jnp.concatenate([tok[:, : half // 2, :], tok[:, half // 2 :, :]], axis=-1)
    pk[...] = packed
    rx[1, t, pl.ds(fr * (1 - t), fr)] = packed[:fr]

    @pl.when(t == 1)
    def _():
        rx[1, 1, fr:] = packed[fr:]

    pl.semaphore_wait(barrier, n - 1)

    partners = [(0, 1), (1, 0), (-1, 0), (1, 1), (-1, 1)]

    def copies(s):
        dh, dt = partners[s]
        other = (t + dt) % n_ta
        to = {"ha": h + dh, "ta": other}
        first = pltpu.make_async_remote_copy(
            src_ref=pk.at[pl.ds(0, fr)],
            dst_ref=rx.at[1 - dh, t, pl.ds(fr * (1 - other), fr)],
            send_sem=tx_a.at[s], recv_sem=rx_a.at[s], device_id=to, device_id_type=MESH,
        )
        second = pltpu.make_async_remote_copy(
            src_ref=pk.at[pl.ds(fr, fr)],
            dst_ref=rx.at[1 - dh, t, pl.ds(fr, fr)],
            send_sem=tx_b.at[s], recv_sem=rx_b.at[s], device_id=to, device_id_type=MESH,
        )
        return first, second, other

    def exists(s, sign):
        dh = partners[s][0] * sign
        return jnp.logical_and(h + dh >= 0, h + dh < n_ha)

    for s in range(5):

        @pl.when(exists(s, 1))
        def _(s=s):
            first, second, other = copies(s)
            first.start()

            @pl.when(other == 1)
            def _():
                second.start()

    get_w_in.wait()
    zero = jnp.zeros((zc, ch), BF16)
    for p in range(3):
        for block in range(4):
            for a1 in range(2):
                for b1 in range(2):
                    dy = (-1 if a1 else 2) if block >= 2 else a1
                    dx = (-1 if b1 else 2) if block % 2 else b1
                    row = p * 16 * zc + block * 4 * zc + (2 * a1 + b1) * zc
                    for a in range(2):
                        for b in range(2):
                            q, r = dy - a + 1, dx - b + 1
                            inside = 0 <= q <= 2 and 0 <= r <= 2
                            piece = w_in[3 * p + q, r * zc : (r + 1) * zc, :] if inside else zero
                            col = (2 * a + b) * ch
                            wexp[row : row + zc, col : col + ch] = piece
    for s in range(5):

        @pl.when(exists(s, -1))
        def _(s=s):
            first, second, _ = copies(s)
            first.wait_recv()

            @pl.when(t == 1)
            def _():
                second.wait_recv()

    rows = frames * cj
    j = lax.broadcasted_iota(jnp.int32, (rows, width), 0) & (cj - 1)
    lane = lax.broadcasted_iota(jnp.int32, (rows, width), 1)
    upper_b = (lane & zc) != 0
    wide = []
    for i in range(3):
        parts = []
        for side in range(n_ta):
            held = rx[i, side].astype(F32)
            parts += [held[:, :, :width], held[:, :, width:]]
        field = jnp.concatenate(parts, axis=1).reshape(rows, width)
        left = jnp.where(j == 0, 0.0, pltpu.roll(field, 1, 0))
        right = jnp.where(j == cj - 1, 0.0, pltpu.roll(field, rows - 1, 0))
        wide.append(jnp.concatenate([field, jnp.where(upper_b, left, right)], axis=-1))
    lane = lax.broadcasted_iota(jnp.int32, (rows, 2 * width), 1)
    upper_a = (lane & (2 * zc)) != 0
    nothing = jnp.zeros_like(wide[0])
    for i in range(3):
        above = wide[i - 1] if i > 0 else nothing
        below = wide[i + 1] if i < 2 else nothing
        crossed = jnp.where(upper_a, above, below)
        patch[i, :, : 2 * width] = wide[i].astype(BF16)
        patch[i, :, 2 * width :] = crossed.astype(BF16)

    def conv(i, lo, count, col0, ncol):
        lhs = jnp.concatenate(
            [patch[i, (lo + p) * cj : (lo + p + count) * cj, :] for p in range(3)], axis=-1
        )
        got = jnp.dot(lhs, wexp[:, col0 : col0 + ncol], preferred_element_type=F32)
        results = []
        for piece in range(ncol // ch):
            value = (got[:, piece * ch : (piece + 1) * ch] + b_in_c).astype(BF16)
            results.append(value)
        return results

    own = conv(1, 2, fr, 0, 4 * ch)
    total = jnp.zeros((1, ch), F32)
    for ab in range(4):
        hid[2:, 1 + ab // 2, ab % 2] = own[ab].reshape(fr, cj, ch)
        total = total + jnp.sum(own[ab].astype(F32), axis=0, keepdims=True)
    cells = 4 * fr * cj
    chan_mean = total * (1.0 / cells)
    squares = jnp.zeros((1, ch), F32)
    for ab in range(4):
        value = hid[2:, 1 + ab // 2, ab % 2].reshape(fr * cj, ch).astype(F32) - chan_mean
        squares = squares + jnp.sum(value * value, axis=0, keepdims=True)
    grouped = split_dot(chan_mean, sums[...]) * (1.0 / members)
    apart = chan_mean - grouped[:, :ch]
    local_m2 = split_dot(squares + cells * apart * apart, sums[:, ch:])
    stat[...] = jnp.concatenate([grouped[:, ch:], local_m2], axis=0)
    gath[me] = stat[...]

    def share(k, c):
        peer = lax.rem(me + k, n)
        pltpu.make_async_remote_copy(
            src_ref=stat, dst_ref=gath.at[me], send_sem=st_tx, recv_sem=st_rx,
            device_id={"ha": peer // n_ta, "ta": peer % n_ta}, device_id_type=MESH,
        ).start()
        return c

    lax.fori_loop(1, n, share, 0, unroll=together)

    early = conv(1, 0, 2, 0, 4 * ch)
    for ab in range(4):
        hid[:2, 1 + ab // 2, ab % 2] = early[ab].reshape(2, cj, ch)
    over = conv(0, 0, ext, 2 * ch, 2 * ch)
    under = conv(2, 0, ext, 0, 2 * ch)
    for b in range(2):
        hid[:, 0, b] = over[b].reshape(ext, cj, ch)
        hid[:, 3, b] = under[b].reshape(ext, cj, ch)

    others = gath.at[pl.ds(0, n - 1)]
    pltpu.make_async_copy(others, others, st_rx).wait()
    pltpu.make_async_copy(others, others, st_tx).wait()
    for s in range(5):

        @pl.when(exists(s, 1))
        def _(s=s):
            first, second, other = copies(s)
            first.wait_send()

            @pl.when(other == 1)
            def _():
                second.wait_send()

    every = gath[...]
    means = every[:, 0:1, :]
    mean = jnp.sum(means, axis=0) * (1.0 / n)
    gap = means - mean[None]
    count = float(cells * members)
    m2 = jnp.sum(every[:, 1:2, :], axis=0) + count * jnp.sum(gap * gap, axis=0)
    mean_c = split_dot(mean, spread[...])
    var_c = split_dot(m2 * (1.0 / (count * n)), spread[...])
    scale_c = lax.rsqrt(var_c + EPS) * gain_c

    edge = lax.broadcasted_iota(jnp.int32, (cj, ch), 0)

    def activate(lf):
        for y in range(4):
            good = jnp.logical_and(
                t * fr + lf >= 2, jnp.logical_and(h * 2 + y >= 1, h * 2 + y < 2 * n_ha + 1)
            )
            live = jnp.where(good, 0.5, 0.0)
            for b in range(2):
                v = (hid[lf, y, b].astype(F32) - mean_c) * scale_c + shift_c
                v = ((v * live) * (1.0 + jnp.tanh(0.5 * v))).astype(BF16)
                for q in range(3):
                    if 0 <= y - q < 2:
                        act[lf, y - q, b * cj : (b + 1) * cj, q * ch : (q + 1) * ch] = v

    lax.fori_loop(0, ext, lambda lf, c: (activate(lf), c)[1], 0)
    for k in range(9):
        pltpu.make_async_copy(w_mid.at[k], wv.at[k], w_sem.at[k]).wait()

    def frame(f, c):
        lhs = jnp.concatenate([act[f + p].reshape(4 * cj, 3 * ch) for p in range(3)], axis=-1)
        rhs = jnp.concatenate(
            [
                jnp.concatenate([wv[k, r * ch : (r + 1) * ch, :] for r in range(3)], axis=-1)
                for k in range(9)
            ],
            axis=0,
        )
        got = jnp.dot(lhs, rhs, preferred_element_type=F32)
        for y in range(2):
            e0, e1, e2 = [got[2 * y * cj : (2 * y + 1) * cj, r * ch : (r + 1) * ch] for r in range(3)]
            o0, o1, o2 = [
                got[(2 * y + 1) * cj : (2 * y + 2) * cj, r * ch : (r + 1) * ch] for r in range(3)
            ]
            from_left = jnp.where(edge == 0, 0.0, pltpu.roll(o0, 1, 0))
            from_right = jnp.where(edge == cj - 1, 0.0, pltpu.roll(e2, cj - 1, 0))
            for b, value in enumerate((from_left + e1 + o2, e0 + o1 + from_right)):
                value = value + (hid[f + 2, y + 1, b].astype(F32) + b_mid_c)
                for piece in range(ch // LANES):
                    cols = slice(piece * LANES, (piece + 1) * LANES)
                    stage[y, piece, pl.ds(b, cj, 2), :] = value[:, cols]
            for piece in range(ch // LANES):
                cols = slice(piece * LANES, (piece + 1) * LANES)
                out[f, y, :, cols] = stage[y, piece].astype(BF16)
        return c

    lax.fori_loop(0, fr, frame, 0)


def body(n_ha, n_ta, latent_tokens, w_in, b_in, gn_gain, gn_shift, w_mid, b_mid):
    frames, half, width = latent_tokens.shape
    ch = b_in.shape[0]
    zc = width // 4
    fr, cj, n = frames // n_ta, half * n_ta, n_ha * n_ta
    vm = pl.BlockSpec(memory_space=pltpu.VMEM)
    far = pl.BlockSpec(memory_space=pl.ANY)
    return pl.pallas_call(
        functools.partial(kernel, n_ha, n_ta),
        out_shape=pltpu.VMEM((fr, 2, 2 * cj, ch), BF16),
        in_specs=[far, far, vm, vm, vm, far, vm],
        out_specs=vm,
        scratch_shapes=[
            pltpu.VMEM((frames, half, width), BF16),
            pltpu.VMEM((9, 3 * zc, ch), BF16),
            pltpu.VMEM((frames, half // 2, 2 * width), BF16),
            pltpu.VMEM((3, n_ta, frames, half // 2, 2 * width), BF16),
            pltpu.VMEM((48 * zc, 4 * ch), BF16),
            pltpu.VMEM((3, frames * cj, 4 * width), BF16),
            pltpu.VMEM((fr + 2, 4, 2, cj, ch), BF16),
            pltpu.VMEM((fr + 2, 2, 2 * cj, 3 * ch), BF16),
            pltpu.VMEM((2, ch // LANES, 2 * cj, LANES), F32),
            pltpu.VMEM((9, 3 * ch, ch), BF16),
            pltpu.VMEM((2, LANES), F32),
            pltpu.VMEM((n, 2, LANES), F32),
            pltpu.VMEM((ch, ch + LANES), BF16),
            pltpu.VMEM((LANES, ch), BF16),
            pltpu.SemaphoreType.DMA((2,)),
            pltpu.SemaphoreType.DMA((9,)),
            pltpu.SemaphoreType.DMA((5,)),
            pltpu.SemaphoreType.DMA((5,)),
            pltpu.SemaphoreType.DMA((5,)),
            pltpu.SemaphoreType.DMA((5,)),
            pltpu.SemaphoreType.DMA,
            pltpu.SemaphoreType.DMA,
        ],
        compiler_params=pltpu.CompilerParams(
            collective_id=0, has_side_effects=True, vmem_limit_bytes=60 * 1024 * 1024
        ),
    )(
        latent_tokens, w_in.reshape(9, 3 * zc, ch), b_in, gn_gain, gn_shift,
        w_mid.reshape(9, 3 * ch, ch), b_mid,
    )


def solution(mesh):
    placed = (P("clip", ("ha", "ta"), None), P(), P(), P(), P(), P(), P())
    return jax.shard_map(
        functools.partial(body, mesh.shape["ha"], mesh.shape["ta"]),
        mesh=mesh,
        in_specs=placed,
        out_specs=P(("clip", "ta"), "ha", None, None),
        check_vma=False,
    )
```
